8 devices in a mesh: dp: 2 (over z, y), cp: 4 (over x, core).
Axes of the slice: x: 2, y: 2, z: 1, core: 2. Of those that a mesh axis runs over, the one named last changes fastest.
Arguments:
- vis_feat: bfloat16 [16, 4096, 1152], P(('dp', 'cp')), parts along dimension 0
- text_emb: bfloat16 [8192, 2048], P(('dp', 'cp')), parts along dimension 0
- img_pos: int32 [16], P('dp'), parts along dimension 0
- grad_y: bfloat16 [8192, 2048], P(('dp', 'cp')), parts along dimension 0
- pn_gain: bfloat16 [1152], replicated
- w_proj: bfloat16 [1152, 2048], replicated
- pre_gain: bfloat16 [2048], replicated
- w_query: bfloat16 [2048, 2048], replicated
- w_key: bfloat16 [2048, 256], replicated
- w_value: bfloat16 [2048, 256], replicated
- q_gain: bfloat16 [256], replicated
- k_gain: bfloat16 [256], replicated
- w_out: bfloat16 [2048, 2048], replicated
- post_gain: bfloat16 [2048], replicated
Outputs:
- output 1: bfloat16 [8192, 2048], P(('dp', 'cp')), parts along dimension 0
- output 2: bfloat16 [8192, 2048], P(('dp', 'cp')), parts along dimension 0
- output 3: bfloat16 [16, 4096, 1152], P(('dp', 'cp')), parts along dimension 0
- output 4: bfloat16 [2304], P('dp'), parts along dimension 0
- output 5: bfloat16 [2304, 2048], P('dp'), parts along dimension 0
- output 6: bfloat16 [4096], P('dp'), parts along dimension 0
- output 7: bfloat16 [4096, 2048], P('dp'), parts along dimension 0
- output 8: bfloat16 [4096, 256], P('dp'), parts along dimension 0
- output 9: bfloat16 [4096, 256], P('dp'), parts along dimension 0
- output 10: bfloat16 [512], P('dp'), parts along dimension 0
- output 11: bfloat16 [512], P('dp'), parts along dimension 0
- output 12: bfloat16 [4096, 2048], P('dp'), parts along dimension 0
- output 13: bfloat16 [4096], P('dp'), parts along dimension 0
There are 2 independent parts. The reference program is written for one: setup_inputs(seed, part) draws one part's arguments, and reference() takes and returns one part's arrays. A program takes and returns all parts, laid end to end along the dimension named above; an argument that names none is the same for every part.
All inputs are finite; a program needn't handle non-finite values.
Results may differ from the reference program's by a relative error of at most 0.02.
Values are sent between devices in bfloat16 or wider.
A program may use at most 1 GiB of HBM per device.

```python
import functools
import jax
import jax.numpy as jnp
from jax import lax

D = 2048
HEADS = 8
KV_HEADS = 1
HEAD = 256
DV = 1152
SEQ_DEV = 1024
IMG_DEV = 2
GROUP = 4
GRID = 64
POOL = 4
SEQ = SEQ_DEV * GROUP
N_IMG = IMG_DEV * GROUP
SIDE = GRID // POOL
BLOCK = SIDE * SIDE
EPS = 1e-6
ROPE_BASE = 1000000.0
ROPE_SCALE = 8.0
NEG_BIG = -1e30


def place_images(rng_key):
    gap_key, perm_key = jax.random.split(rng_key)
    first_start = SEQ_DEV - BLOCK // 2
    spare = SEQ - N_IMG * BLOCK - first_start
    raw_gap = jax.random.randint(gap_key, (N_IMG,), 0, 8)
    weight = raw_gap * raw_gap * raw_gap
    gap_total = jnp.maximum(jnp.sum(weight), 1)
    gap_rows = spare * weight // gap_total
    slot_start = first_start + jnp.arange(N_IMG) * BLOCK + jnp.cumsum(gap_rows) - gap_rows
    slot_order = jax.random.permutation(perm_key, N_IMG)
    return slot_start[slot_order].astype(jnp.int32)


def draw_normal(rng_key, arr_shape, std_scale):
    return (jax.random.normal(rng_key, arr_shape, jnp.float32) * std_scale).astype(jnp.bfloat16)


def setup_inputs(seed: int = 0, part: int = 0) -> dict:
    base_key = jax.random.key(seed)
    part_keys = jax.random.split(jax.random.fold_in(base_key, part), 4)
    weight_keys = jax.random.split(jax.random.key(seed + 1), 10)
    return {
        'vis_feat': draw_normal(part_keys[0], (N_IMG, GRID * GRID, DV), 1.0),
        'text_emb': draw_normal(part_keys[1], (SEQ, D), 1.0),
        'img_pos': place_images(part_keys[2]),
        'grad_y': draw_normal(part_keys[3], (SEQ, D), 1.0),
        'pn_gain': draw_normal(weight_keys[0], (DV,), 0.3),
        'w_proj': draw_normal(weight_keys[1], (DV, D), DV ** -0.5),
        'pre_gain': draw_normal(weight_keys[2], (D,), 0.3),
        'w_query': draw_normal(weight_keys[3], (D, HEADS * HEAD), D ** -0.5),
        'w_key': draw_normal(weight_keys[4], (D, KV_HEADS * HEAD), D ** -0.5),
        'w_value': draw_normal(weight_keys[5], (D, KV_HEADS * HEAD), D ** -0.5),
        'q_gain': draw_normal(weight_keys[6], (HEAD,), 0.3),
        'k_gain': draw_normal(weight_keys[7], (HEAD,), 0.3),
        'w_out': draw_normal(weight_keys[8], (HEADS * HEAD, D), (HEADS * HEAD) ** -0.5),
        'post_gain': draw_normal(weight_keys[9], (D,), 0.3),
    }


def rms_scale(values, gain_vec):
    wide_vals = values.astype(jnp.float32)
    mean_sq = jnp.mean(wide_vals * wide_vals, axis=-1, keepdims=True)
    return wide_vals * lax.rsqrt(mean_sq + EPS) * (1.0 + gain_vec.astype(jnp.float32))


def rope_tables(positions):
    inv_freq = ROPE_BASE ** (-jnp.arange(0, HEAD, 2).astype(jnp.float32) / HEAD)
    rot_angle = (positions.astype(jnp.float32) / ROPE_SCALE)[:, None] * inv_freq[None, :]
    rot_angle = jnp.concatenate([rot_angle, rot_angle], axis=-1)
    return jnp.cos(rot_angle)[:, None, :], jnp.sin(rot_angle)[:, None, :]


def apply_rope(values, cos_t, sin_t):
    half_dim = values.shape[-1] // 2
    rotated = jnp.concatenate([-values[..., half_dim:], values[..., :half_dim]], axis=-1)
    return values * cos_t + rotated * sin_t


def project(vis_feat, pn_gain, w_proj):
    img_count = vis_feat.shape[0]
    patch_grid = vis_feat.reshape(img_count, SIDE, POOL, SIDE, POOL, DV).astype(jnp.float32)
    pooled = (jnp.sum(patch_grid, axis=(2, 4)) / (POOL * POOL)).astype(jnp.bfloat16)
    normed = rms_scale(pooled.reshape(img_count * BLOCK, DV), pn_gain).astype(jnp.bfloat16)
    return jnp.dot(normed, w_proj, preferred_element_type=jnp.float32).astype(jnp.bfloat16)


def attend_block(q_blk, start_blk, blk_index, k_heads, v_heads):
    groups = HEADS // KV_HEADS
    q_pos = blk_index * SEQ_DEV + jnp.arange(SEQ_DEV)
    key_pos = jnp.arange(SEQ)
    in_image = (start_blk[:, None] >= 0) & (key_pos[None, :] >= start_blk[:, None]) & (key_pos[None, :] < start_blk[:, None] + BLOCK)
    visible = (key_pos[None, :] <= q_pos[:, None]) | in_image
    q_grp = q_blk.reshape(SEQ_DEV, KV_HEADS, groups, HEAD).astype(jnp.float32)
    scores = jnp.einsum('qkgd,skd->kgqs', q_grp, k_heads.astype(jnp.float32)) * HEAD ** -0.5
    scores = jnp.where(visible[None, None], scores, NEG_BIG)
    prob_lo = jax.nn.softmax(scores, axis=-1).astype(jnp.bfloat16)
    attn_blk = jnp.einsum('kgqs,skd->qkgd', prob_lo.astype(jnp.float32), v_heads.astype(jnp.float32))
    return attn_blk.astype(jnp.bfloat16).reshape(SEQ_DEV, HEADS * HEAD)


def forward(vis_feat, text_emb, pn_gain, w_proj, pre_gain, w_query, w_key, w_value, q_gain, k_gain, w_out, post_gain, img_pos):
    soft_tok = project(vis_feat, pn_gain, w_proj)
    img_rows = (img_pos[:, None] + jnp.arange(BLOCK)[None, :]).reshape(-1)
    merged = text_emb.at[img_rows].set(soft_tok)
    starts = jnp.full((SEQ,), -1, jnp.int32).at[img_rows].set(jnp.repeat(img_pos, BLOCK))
    hidden = rms_scale(merged, pre_gain).astype(jnp.bfloat16)
    q_raw = jnp.dot(hidden, w_query, preferred_element_type=jnp.float32).astype(jnp.bfloat16).reshape(SEQ, HEADS, HEAD)
    k_raw = jnp.dot(hidden, w_key, preferred_element_type=jnp.float32).astype(jnp.bfloat16).reshape(SEQ, KV_HEADS, HEAD)
    v_heads = jnp.dot(hidden, w_value, preferred_element_type=jnp.float32).astype(jnp.bfloat16).reshape(SEQ, KV_HEADS, HEAD)
    cos_t, sin_t = rope_tables(jnp.arange(SEQ))
    q_heads = apply_rope(rms_scale(q_raw, q_gain), cos_t, sin_t).astype(jnp.bfloat16)
    k_heads = apply_rope(rms_scale(k_raw, k_gain), cos_t, sin_t).astype(jnp.bfloat16)
    block_fn = jax.checkpoint(attend_block)
    attn_out = lax.map(lambda blk_args: block_fn(blk_args[0], blk_args[1], blk_args[2], k_heads, v_heads), (q_heads.reshape(GROUP, SEQ_DEV, HEADS, HEAD), starts.reshape(GROUP, SEQ_DEV), jnp.arange(GROUP)))
    attn_out = attn_out.reshape(SEQ, HEADS * HEAD)
    proj_out = jnp.dot(attn_out, w_out, preferred_element_type=jnp.float32).astype(jnp.bfloat16)
    return (merged.astype(jnp.float32) + rms_scale(proj_out, post_gain)).astype(jnp.bfloat16)


def reference(vis_feat, text_emb, img_pos, grad_y, pn_gain, w_proj, pre_gain, w_query, w_key, w_value, q_gain, k_gain, w_out, post_gain):
    y_out, pullback = jax.vjp(functools.partial(forward, img_pos=img_pos), vis_feat, text_emb, pn_gain, w_proj, pre_gain, w_query, w_key, w_value, q_gain, k_gain, w_out, post_gain)
    grad_list = pullback(grad_y)
    return (y_out, grad_list[1], grad_list[0], grad_list[2], grad_list[3], grad_list[4], grad_list[5], grad_list[6], grad_list[7], grad_list[8], grad_list[9], grad_list[10], grad_list[11])
```

```python
import functools
import jax
import jax.numpy as jnp
from jax import lax
from jax.experimental import pallas as pl
from jax.experimental.pallas import tpu as pltpu
from jax.sharding import PartitionSpec as P

GRID = 64
POOL = 4
SIDE = GRID // POOL
BLOCK = SIDE * SIDE
EPS = 1e-6
ROPE_BASE = 1000000.0
ROPE_SCALE = 8.0
NEG_BIG = -1e30
HEAD = 256
HALF = HEAD // 2
BQ = 512
BK = 512
BM = 256
RB = 256
VMEM_LIMIT = 60 * 1024 * 1024
F32 = jnp.float32
BF16 = jnp.bfloat16


def params(sem):
    return pltpu.CompilerParams(dimension_semantics=sem, vmem_limit_bytes=VMEM_LIMIT)


def cost(flops, nbytes):
    return pl.CostEstimate(flops=int(flops), bytes_accessed=int(nbytes), transcendentals=0)


def dot(a, b):
    return jnp.dot(a, b, preferred_element_type=F32)


def dot_t(a, b):
    return lax.dot_general(a, b, (((1,), (1,)), ((), ())), preferred_element_type=F32)


def iota(shape, axis):
    return lax.broadcasted_iota(jnp.int32, shape, axis)


def wide(stat, width):
    return jnp.concatenate([stat] * (width // 128), axis=1)


def pool_kernel(vis_ref, out_ref):
    rows, cols = SIDE, POOL * GRID
    patch = iota((rows, cols), 1) % GRID
    sel = (patch // POOL == iota((rows, cols), 0)).astype(BF16)
    for i in range(vis_ref.shape[1] // cols):
        total = dot(sel, vis_ref[0, i * cols:(i + 1) * cols, :])
        out_ref[i * rows:(i + 1) * rows, :] = (total / (POOL * POOL)).astype(BF16)


def pool_patches(vis_loc):
    n_img, n_patch, dim = vis_loc.shape
    bands = 4
    steps = SIDE // bands
    return pl.pallas_call(
        pool_kernel,
        out_shape=jax.ShapeDtypeStruct((n_img * BLOCK, dim), BF16),
        grid=(n_img, steps),
        in_specs=[pl.BlockSpec((1, bands * POOL * GRID, dim), lambda n, i: (n, i, 0))],
        out_specs=pl.BlockSpec((bands * SIDE, dim), lambda n, i: (n * steps + i, 0)),
        compiler_params=params(("arbitrary", "arbitrary")),
        cost_estimate=cost(4e9, n_img * n_patch * dim * 2),
        name="pool",
    )(vis_loc)


def unpool_kernel(d_ref, out_ref):
    rows, cols = POOL * GRID, SIDE
    patch = iota((rows, cols), 0) % GRID
    sel = (patch // POOL == iota((rows, cols), 1)).astype(BF16)
    for i in range(out_ref.shape[1] // rows):
        band = (d_ref[i * cols:(i + 1) * cols, :].astype(F32) / (POOL * POOL)).astype(BF16)
        out_ref[0, i * rows:(i + 1) * rows, :] = dot(sel, band).astype(BF16)


def unpool_grad(d_pooled, n_img):
    dim = d_pooled.shape[1]
    bands = 4
    steps = SIDE // bands
    return pl.pallas_call(
        unpool_kernel,
        out_shape=jax.ShapeDtypeStruct((n_img, GRID * GRID, dim), BF16),
        grid=(n_img, steps),
        in_specs=[pl.BlockSpec((bands * SIDE, dim), lambda n, i: (n * steps + i, 0))],
        out_specs=pl.BlockSpec((1, bands * POOL * GRID, dim), lambda n, i: (n, i, 0)),
        compiler_params=params(("arbitrary", "arbitrary")),
        cost_estimate=cost(4e9, n_img * GRID * GRID * dim * 2),
        name="unpool",
    )(d_pooled)


def rms(x):
    return lax.rsqrt(jnp.mean(x * x, axis=-1, keepdims=True) + EPS)


def norm_rope(raw, gain1, cos_t, sin_t):
    x = raw.astype(F32)
    x = x * rms(x) * gain1
    lo, hi = x[:, :HALF], x[:, HALF:]
    return (lo * cos_t - hi * sin_t).astype(BF16), (hi * cos_t + lo * sin_t).astype(BF16)


def norm_rope_grad(d_out, raw, gain1, cos_t, sin_t):
    d = d_out.astype(F32)
    lo, hi = d[:, :HALF], d[:, HALF:]
    d = jnp.concatenate([lo * cos_t + hi * sin_t, hi * cos_t - lo * sin_t], axis=1)
    x = raw.astype(F32)
    r = rms(x)
    xr = x * r
    dg = d * gain1
    d_raw = r * (dg - xr * jnp.mean(xr * dg, axis=-1, keepdims=True))
    return d_raw.astype(BF16), jnp.sum(d * xr, axis=0, keepdims=True)


def qkv_kernel(meta, text_own, text_mate, soft_a, soft_b, pre1, wq, wk, wv, qg1, kg1, cos_ref, sin_ref,
               x_out, hid_out, qraw_out, q_out, kraw_out, k_out, v_out, x_scr):
    i = pl.program_id(0)
    half = pl.num_programs(0) // 2
    own = (i < half) == (meta[0, 0] == 1)

    @pl.when(own)
    def _():
        x_scr[...] = text_own[...]

    @pl.when(jnp.logical_not(own))
    def _():
        x_scr[...] = text_mate[...]

    for slot, soft in ((0, soft_a), (1, soft_b)):
        off = meta[3 + slot, i]

        @pl.when(off < RB)
        def _():
            src = iota((RB, BLOCK), 0) - off
            pick = (src == iota((RB, BLOCK), 1)).astype(BF16)
            row = iota((RB, 1), 0) - off
            inside = (row >= 0) & (row < BLOCK)
            x_scr[...] = jnp.where(inside, dot(pick, soft[...]).astype(BF16), x_scr[...])

    x_out[...] = x_scr[...]
    x = x_scr[...].astype(F32)
    hid_out[...] = (x * rms(x) * pre1[...]).astype(BF16)
    hid = hid_out[...]
    qraw_out[...] = dot(hid, wq[...]).astype(BF16)
    kraw_out[...] = dot(hid, wk[...]).astype(BF16)
    v_out[...] = dot(hid, wv[...]).astype(BF16)
    cos_t, sin_t = cos_ref[...], sin_ref[...]
    lo, hi = norm_rope(kraw_out[...], kg1[...], cos_t, sin_t)
    k_out[:, :HALF] = lo
    k_out[:, HALF:] = hi
    for h in range(q_out.shape[1] // HEAD):
        lo, hi = norm_rope(qraw_out[:, h * HEAD:(h + 1) * HEAD], qg1[...], cos_t, sin_t)
        q_out[:, h * HEAD:h * HEAD + HALF] = (lo * 0.0625).astype(BF16)
        q_out[:, h * HEAD + HALF:(h + 1) * HEAD] = (hi * 0.0625).astype(BF16)


def qkv_call(meta, text_own, text_mate, soft_all, pre1, wq, wk, wv, qg1, kg1, cos_t, sin_t):
    rows, dim = text_own.shape
    steps = 2 * rows // RB
    half = steps // 2
    width = wq.shape[1]

    def own_map(i, meta):
        is_lo = meta[0, 0] == 1
        return jnp.where(is_lo, jnp.minimum(i, half - 1), jnp.maximum(i - half, 0)), 0

    def mate_map(i, meta):
        is_lo = meta[0, 0] == 1
        return jnp.where(is_lo, jnp.maximum(i - half, 0), jnp.minimum(i, half - 1)), 0

    def row(w):
        return pl.BlockSpec((RB, w), lambda i, meta: (i, 0))

    def whole(a):
        return pl.BlockSpec(a.shape, lambda i, meta: (0,) * a.ndim, pipeline_mode=pl.Buffered(1))

    def struct(w):
        return jax.ShapeDtypeStruct((2 * rows, w), BF16)

    return pl.pallas_call(
        qkv_kernel,
        out_shape=[struct(dim), struct(dim), struct(width), struct(width), struct(HEAD), struct(HEAD), struct(HEAD)],
        grid_spec=pltpu.PrefetchScalarGridSpec(
            num_scalar_prefetch=1, grid=(steps,),
            in_specs=[pl.BlockSpec((RB, dim), own_map), pl.BlockSpec((RB, dim), mate_map),
                      pl.BlockSpec((BLOCK, dim), lambda i, meta: (meta[1, i], 0)),
                      pl.BlockSpec((BLOCK, dim), lambda i, meta: (meta[2, i], 0)),
                      whole(pre1), whole(wq), whole(wk), whole(wv), whole(qg1), whole(kg1), row(HALF), row(HALF)],
            out_specs=[row(dim), row(dim), row(width), row(width), row(HEAD), row(HEAD), row(HEAD)],
            scratch_shapes=[pltpu.VMEM((RB, dim), BF16)]),
        compiler_params=params(("arbitrary",)),
        cost_estimate=cost(4 * rows * dim * (width + 2 * HEAD), 60e6),
        name="qkv",
    )(meta, text_own, text_mate, soft_all, soft_all, pre1, wq, wk, wv, qg1, kg1, cos_t, sin_t)


def fwd_kernel(span, q_ref, kt_ref, v_ref, lim_ref, o_ref, lse_ref, acc, m_scr, l_scr):
    b = pl.program_id(0)
    q = q_ref[...]
    acc[...] = jnp.zeros_like(acc)
    m_scr[...] = jnp.full_like(m_scr, NEG_BIG)
    l_scr[...] = jnp.zeros_like(l_scr)

    def step(off, bk, masked):
        off = pl.multiple_of(off, bk)
        s = dot(q, kt_ref[:, pl.ds(off, bk)])
        if masked:
            key = off + iota(s.shape, 1)
            s = jnp.where(key < wide(lim_ref[...], bk), s, NEG_BIG)
        m_old = m_scr[...]
        m_new = jnp.maximum(m_old, jnp.max(s, axis=1, keepdims=True))
        p = jnp.exp(s - wide(m_new, bk))
        alpha = jnp.exp(m_old - m_new)
        l_scr[...] = alpha * l_scr[...] + jnp.sum(p, axis=1, keepdims=True)
        m_scr[...] = m_new
        acc[...] = acc[...] * wide(alpha, HEAD) + dot(p.astype(BF16), v_ref[pl.ds(off, bk), :])

    @pl.loop(0, span[0, b])
    def _(j):
        step(j * BK, BK, False)

    @pl.loop(span[1, b], span[2, b])
    def _(j):
        step(j * BM, BM, True)

    l = l_scr[...]
    o_ref[...] = (acc[...] / wide(l, HEAD)).astype(BF16)
    lse_ref[0] = (m_scr[...] + jnp.log(l)).T[0:1, :]


def fwd_call(span, q, kt, v, lim):
    rows, width = q.shape
    heads = width // HEAD
    seq = v.shape[0]
    return pl.pallas_call(
        fwd_kernel,
        out_shape=[jax.ShapeDtypeStruct((rows, width), BF16), jax.ShapeDtypeStruct((heads, 1, rows), F32)],
        grid_spec=pltpu.PrefetchScalarGridSpec(
            num_scalar_prefetch=1, grid=(rows // BQ, heads),
            in_specs=[pl.BlockSpec((BQ, HEAD), lambda b, h, s: (b, h)),
                      pl.BlockSpec((HEAD, seq), lambda b, h, s: (0, 0)),
                      pl.BlockSpec((seq, HEAD), lambda b, h, s: (0, 0)),
                      pl.BlockSpec((BQ, 128), lambda b, h, s: (b, 0))],
            out_specs=[pl.BlockSpec((BQ, HEAD), lambda b, h, s: (b, h)),
                       pl.BlockSpec((1, 1, BQ), lambda b, h, s: (h, 0, b))],
            scratch_shapes=[pltpu.VMEM((BQ, HEAD), F32), pltpu.VMEM((BQ, 128), F32), pltpu.VMEM((BQ, 128), F32)]),
        compiler_params=params(("arbitrary", "arbitrary")),
        cost_estimate=cost(2 * rows * seq * width, 30e6),
        name="attn_fwd",
    )(span, q, kt, v, lim)


def bwd_kernel(span, q_ref, do_ref, k_ref, kt_ref, v_ref, lim_ref, lse_ref, delta_ref, qraw_ref, qg1, cos_ref, sin_ref,
               dqraw_ref, gq_ref, dk_ref, dv_ref, qt, dot_scr, dqt):
    b, h = pl.program_id(0), pl.program_id(1)

    @pl.when((b == 0) & (h == 0))
    def _():
        dk_ref[...] = jnp.zeros_like(dk_ref)
        dv_ref[...] = jnp.zeros_like(dv_ref)
        gq_ref[...] = jnp.zeros_like(gq_ref)

    qt[...] = q_ref[...].astype(F32).T.astype(BF16)
    dot_scr[...] = do_ref[...].astype(F32).T.astype(BF16)
    dqt[...] = jnp.zeros_like(dqt)
    lse = lse_ref[0]
    delta = delta_ref[0]

    def step(off, bk, masked):
        off = pl.multiple_of(off, bk)
        rows = pl.ds(off, bk)
        p = jnp.exp(dot(k_ref[rows, :], qt[...]) - lse)
        if masked:
            p = jnp.where(off + iota(p.shape, 0) < lim_ref[...], p, 0.0)
        ds = (p * (dot(v_ref[rows, :], dot_scr[...]) - delta)).astype(BF16)
        dv_ref[rows, :] += dot(p.astype(BF16), do_ref[...])
        dk_ref[rows, :] += dot(ds, q_ref[...])
        dqt[...] += dot(kt_ref[:, rows], ds)

    @pl.loop(0, span[0, b])
    def _(j):
        step(j * BK, BK, False)

    @pl.loop(span[1, b], span[2, b])
    def _(j):
        step(j * BM, BM, True)

    d_q = (dqt[...].T * 0.0625).astype(BF16)
    d_raw, g_part = norm_rope_grad(d_q, qraw_ref[...], qg1[...], cos_ref[...], sin_ref[...])
    dqraw_ref[...] = d_raw
    gq_ref[...] += g_part


def bwd_call(span, q, d_o, k, kt, v, lim_t, lse, delta, q_raw, qg1, cos_t, sin_t):
    rows, width = q.shape
    heads = width // HEAD
    seq = v.shape[0]
    tile = pl.BlockSpec((BQ, HEAD), lambda b, h, s: (b, h))
    keys = pl.BlockSpec((seq, HEAD), lambda b, h, s: (0, 0))
    stat = pl.BlockSpec((1, 1, BQ), lambda b, h, s: (h, 0, b))
    rot = pl.BlockSpec((BQ, HALF), lambda b, h, s: (b, 0))
    return pl.pallas_call(
        bwd_kernel,
        out_shape=[jax.ShapeDtypeStruct((rows, width), BF16), jax.ShapeDtypeStruct((1, HEAD), F32),
                   jax.ShapeDtypeStruct((seq, HEAD), F32), jax.ShapeDtypeStruct((seq, HEAD), F32)],
        grid_spec=pltpu.PrefetchScalarGridSpec(
            num_scalar_prefetch=1, grid=(rows // BQ, heads),
            in_specs=[tile, tile, keys, pl.BlockSpec((HEAD, seq), lambda b, h, s: (0, 0)), keys,
                      pl.BlockSpec((1, BQ), lambda b, h, s: (0, b)), stat, stat, tile,
                      pl.BlockSpec((1, HEAD), lambda b, h, s: (0, 0)), rot, rot],
            out_specs=[tile, pl.BlockSpec((1, HEAD), lambda b, h, s: (0, 0)), keys, keys],
            scratch_shapes=[pltpu.VMEM((HEAD, BQ), BF16), pltpu.VMEM((HEAD, BQ), BF16), pltpu.VMEM((HEAD, BQ), F32)]),
        compiler_params=params(("arbitrary", "arbitrary")),
        cost_estimate=cost(5 * rows * seq * width, 50e6),
        name="attn_bwd",
    )(span, q, d_o, k, kt, v, lim_t, lse, delta, q_raw, qg1, cos_t, sin_t)


def out_kernel(meta, o_ref, x_ref, dy_own, dy_mate, wo, post1, y_ref, da_ref, do_ref, delta_ref, gpost_ref, dy_scr):
    i = pl.program_id(0)
    half = pl.num_programs(0) // 2
    own = (i < half) == (meta[0, 0] == 1)

    @pl.when(i == 0)
    def _():
        gpost_ref[...] = jnp.zeros_like(gpost_ref)

    @pl.when(own)
    def _():
        dy_scr[...] = dy_own[...]

    @pl.when(jnp.logical_not(own))
    def _():
        dy_scr[...] = dy_mate[...]

    a = dot(o_ref[...], wo[...]).astype(BF16).astype(F32)
    r = rms(a)
    ar = a * r

    @pl.when(own)
    def _():
        y_ref[...] = (x_ref[...].astype(F32) + ar * post1[...]).astype(BF16)

    dy = dy_scr[...].astype(F32)
    gpost_ref[...] += jnp.sum(dy * ar, axis=0, keepdims=True)
    dg = dy * post1[...]
    da_ref[...] = (r * (dg - ar * jnp.mean(ar * dg, axis=-1, keepdims=True))).astype(BF16)
    do_ref[...] = dot_t(da_ref[...], wo[...]).astype(BF16)
    cols = []
    for h in range(o_ref.shape[1] // HEAD):
        c = slice(h * HEAD, (h + 1) * HEAD)
        cols.append(jnp.sum(do_ref[:, c].astype(F32) * o_ref[:, c].astype(F32), axis=-1, keepdims=True))
    delta_ref[...] = jnp.concatenate(cols, axis=1)


def own_maps(half):
    def own_map(i, meta):
        is_lo = meta[0, 0] == 1
        return jnp.where(is_lo, jnp.minimum(i, half - 1), jnp.maximum(i - half, 0)), 0

    def mate_map(i, meta):
        is_lo = meta[0, 0] == 1
        return jnp.where(is_lo, jnp.maximum(i - half, 0), jnp.minimum(i, half - 1)), 0

    return own_map, mate_map


def out_call(meta, o, x, dy_own, dy_mate, wo, post1):
    rows, width = o.shape
    dim = wo.shape[1]
    steps = rows // RB
    own_map, mate_map = own_maps(steps // 2)
    row = lambda w: pl.BlockSpec((RB, w), lambda i, meta: (i, 0))
    heads = width // HEAD
    return pl.pallas_call(
        out_kernel,
        out_shape=[jax.ShapeDtypeStruct(dy_own.shape, BF16), jax.ShapeDtypeStruct((rows, dim), BF16),
                   jax.ShapeDtypeStruct((rows, width), BF16), jax.ShapeDtypeStruct((rows, heads), F32),
                   jax.ShapeDtypeStruct((1, dim), F32)],
        grid_spec=pltpu.PrefetchScalarGridSpec(
            num_scalar_prefetch=1, grid=(steps,),
            in_specs=[row(width), row(dim), pl.BlockSpec((RB, dim), own_map), pl.BlockSpec((RB, dim), mate_map),
                      pl.BlockSpec(wo.shape, lambda i, meta: (0, 0), pipeline_mode=pl.Buffered(1)),
                      pl.BlockSpec((1, dim), lambda i, meta: (0, 0))],
            out_specs=[pl.BlockSpec((RB, dim), own_map), row(dim), row(width), row(heads),
                       pl.BlockSpec((1, dim), lambda i, meta: (0, 0))],
            scratch_shapes=[pltpu.VMEM((RB, dim), BF16)]),
        compiler_params=params(("arbitrary",)),
        cost_estimate=cost(4 * rows * dim * width, 60e6),
        name="out_proj",
    )(meta, o, x, dy_own, dy_mate, wo, post1)


def hid_kernel(meta, dq_ref, dk_mine, dv_mine, dkv_theirs, kraw_ref, cos_ref, sin_ref, kg1, wq, wk, wv, x_ref, pre1,
               dy_own, dy_mate, lim_ref, dtext_ref, dm_ref, dk_ref, dv_ref, gpre_ref, gk_ref, dy_scr):
    i = pl.program_id(0)
    half = pl.num_programs(0) // 2
    own = (i < half) == (meta[0, 0] == 1)

    @pl.when(i == 0)
    def _():
        gpre_ref[...] = jnp.zeros_like(gpre_ref)
        gk_ref[...] = jnp.zeros_like(gk_ref)

    @pl.when(own)
    def _():
        dy_scr[...] = dy_own[...]

    @pl.when(jnp.logical_not(own))
    def _():
        dy_scr[...] = dy_mate[...]

    d_k = (dk_mine[...] + dkv_theirs[:, :HEAD]).astype(BF16)
    dv_ref[...] = (dv_mine[...] + dkv_theirs[:, HEAD:]).astype(BF16)
    dk_ref[...], g_part = norm_rope_grad(d_k, kraw_ref[...], kg1[...], cos_ref[...], sin_ref[...])
    gk_ref[...] += g_part
    dh = dot_t(dq_ref[...], wq[...]) + dot_t(dk_ref[...], wk[...]) + dot_t(dv_ref[...], wv[...])
    dh = dh.astype(BF16).astype(F32)
    x = x_ref[...].astype(F32)
    r = rms(x)
    xr = x * r
    gpre_ref[...] += jnp.sum(dh * xr, axis=0, keepdims=True)
    dg = dh * pre1[...]
    dx = (r * (dg - xr * jnp.mean(xr * dg, axis=-1, keepdims=True))).astype(BF16).astype(F32)
    dm = (dy_scr[...].astype(F32) + dx).astype(BF16)
    dm_ref[...] = dm

    @pl.when(own)
    def _():
        dtext_ref[...] = jnp.where(lim_ref[:, :1] > 0, jnp.zeros_like(dm), dm)


def hid_call(meta, dq, dk_part, dv_part, dkv_theirs, k_raw, cos_t, sin_t, kg1, wq, wk, wv, x, pre1, dy_own, dy_mate, img_flag):
    rows, width = dq.shape
    dim = wq.shape[0]
    steps = rows // RB
    own_map, mate_map = own_maps(steps // 2)
    row = lambda w: pl.BlockSpec((RB, w), lambda i, meta: (i, 0))
    part = pl.BlockSpec((RB, HEAD), lambda i, meta: (meta[5, i], 0))
    whole = lambda a: pl.BlockSpec(a.shape, lambda i, meta: (0, 0), pipeline_mode=pl.Buffered(1))
    return pl.pallas_call(
        hid_kernel,
        out_shape=[jax.ShapeDtypeStruct(dy_own.shape, BF16), jax.ShapeDtypeStruct((rows, dim), BF16),
                   jax.ShapeDtypeStruct((rows, HEAD), BF16), jax.ShapeDtypeStruct((rows, HEAD), BF16),
                   jax.ShapeDtypeStruct((1, dim), F32), jax.ShapeDtypeStruct((1, HEAD), F32)],
        grid_spec=pltpu.PrefetchScalarGridSpec(
            num_scalar_prefetch=1, grid=(steps,),
            in_specs=[row(width), part, part, row(2 * HEAD), row(HEAD), row(HALF), row(HALF), whole(kg1),
                      whole(wq), whole(wk), whole(wv), row(dim), whole(pre1),
                      pl.BlockSpec((RB, dim), own_map), pl.BlockSpec((RB, dim), mate_map), row(128)],
            out_specs=[pl.BlockSpec((RB, dim), own_map), row(dim), row(HEAD), row(HEAD),
                       pl.BlockSpec((1, dim), lambda i, meta: (0, 0)), pl.BlockSpec((1, HEAD), lambda i, meta: (0, 0))],
            scratch_shapes=[pltpu.VMEM((RB, dim), BF16)]),
        compiler_params=params(("arbitrary",)),
        cost_estimate=cost(2 * rows * dim * (width + 2 * HEAD), 60e6),
        name="hid_bwd",
    )(meta, dq, dk_part, dv_part, dkv_theirs, k_raw, cos_t, sin_t, kg1, wq, wk, wv, x, pre1, dy_own, dy_mate, img_flag)


def pick_kernel(meta, mine0, theirs0, mine1, theirs1, out_ref, blk):
    n = pl.program_id(0)
    off = meta[2, n]
    for slot, mine, theirs in ((0, mine0, theirs0), (1, mine1, theirs1)):
        is_mine = meta[3 + slot, n] == 1

        @pl.when(is_mine)
        def _():
            blk[...] = mine[...]

        @pl.when(jnp.logical_not(is_mine))
        def _():
            blk[...] = theirs[...]

        src = iota((BLOCK, RB), 0) + off - slot * RB
        pick = (src == iota((BLOCK, RB), 1)).astype(BF16)
        if slot == 0:
            out_ref[...] = dot(pick, blk[...]).astype(BF16)
        else:
            out_ref[...] = jnp.where(src[:, :1] >= 0, dot(pick, blk[...]).astype(BF16), out_ref[...])


def pick_call(meta, mine, theirs):
    dim = mine.shape[1]
    n_img = meta.shape[1]
    at = lambda slot: pl.BlockSpec((RB, dim), lambda n, meta: (meta[slot, n], 0))
    return pl.pallas_call(
        pick_kernel,
        out_shape=jax.ShapeDtypeStruct((n_img * BLOCK, dim), BF16),
        grid_spec=pltpu.PrefetchScalarGridSpec(
            num_scalar_prefetch=1, grid=(n_img,),
            in_specs=[at(0), at(0), at(1), at(1)],
            out_specs=pl.BlockSpec((BLOCK, dim), lambda n, meta: (n, 0)),
            scratch_shapes=[pltpu.VMEM((RB, dim), BF16)]),
        compiler_params=params(("arbitrary",)),
        cost_estimate=cost(4 * n_img * BLOCK * RB * dim, 20e6),
        name="pick_rows",
    )(meta, mine, theirs, mine, theirs)


def gain_norm(values, gain_vec):
    wide = values.astype(F32)
    return (wide * lax.rsqrt(jnp.mean(wide * wide, axis=-1, keepdims=True) + EPS) * (1.0 + gain_vec)).astype(BF16)


def tdot(a, b):
    return lax.dot_general(a, b, (((0,), (0,)), ((), ())), preferred_element_type=F32)


def solution(mesh):
    n_dev = mesh.shape['cp']
    seq_spec = P(('dp', 'cp'))
    part_spec = P('dp')
    rep_spec = P()
    across = [(i, n_dev - 1 - i) for i in range(n_dev)]
    beside = [(i, i ^ 1) for i in range(n_dev)]

    def swap_x(v):
        return lax.ppermute(v, 'cp', across)

    def swap_c(v):
        return lax.ppermute(v, 'cp', beside)

    def device_body(vis_loc, text_loc, img_pos, grad_y, pn_gain, w_proj, pre_gain, w_query, w_key, w_value, q_gain, k_gain, w_out, post_gain):
        dev = lax.axis_index('cp')
        seq_loc, dim = text_loc.shape
        seq = seq_loc * n_dev
        mate = n_dev - 1 - dev
        lo_dev, hi_dev = jnp.minimum(dev, mate), jnp.maximum(dev, mate)
        is_lo = dev < mate
        my_set = lo_dev
        first = my_set == 0
        pre1 = (1.0 + pre_gain.astype(F32))[None]
        post1 = (1.0 + post_gain.astype(F32))[None]
        qg1 = (1.0 + q_gain.astype(F32))[None]
        kg1 = (1.0 + k_gain.astype(F32))[None]

        blocks = 2 * seq_loc // RB
        half = blocks // 2
        blk = jnp.arange(blocks)
        blk_base = jnp.where(blk < half, lo_dev * seq_loc + blk * RB, hi_dev * seq_loc + (blk - half) * RB)
        row = jnp.arange(2 * seq_loc)
        pos = jnp.where(row < seq_loc, lo_dev * seq_loc + row, (hi_dev - 1) * seq_loc + row)
        img = jnp.arange(img_pos.shape[0])
        img_dev = img // 2
        img_set = jnp.minimum(img_dev, n_dev - 1 - img_dev)
        img_slot = jnp.where(img_set == my_set, 0, 4) + jnp.where(img_dev >= n_dev // 2, 2, 0) + img % 2
        rel = img_pos[None, :] - blk_base[:, None]
        hit0 = (rel > -BLOCK) & (rel <= 0)
        hit1 = (rel > 0) & (rel < RB)
        pick_of = lambda hit: jnp.sum(jnp.where(hit, img_slot[None], 0), axis=1)
        off_of = lambda hit: jnp.where(jnp.any(hit, axis=1), jnp.sum(jnp.where(hit, rel, 0), axis=1), seq)
        meta = jnp.stack([jnp.where(is_lo, 1, 0) + 0 * blk, pick_of(hit0), pick_of(hit1), off_of(hit0), off_of(hit1),
                          blk_base // RB]).astype(jnp.int32)
        offset = pos[:, None] - img_pos[None, :]
        in_blk = (offset >= 0) & (offset < BLOCK)
        lim = jnp.maximum(pos + 1, jnp.max(jnp.where(in_blk, img_pos[None, :] + BLOCK, 0), axis=1)).astype(jnp.int32)
        is_img = jnp.any(in_blk, axis=1).astype(jnp.int32)
        q_base = pos[::BQ]
        span = jnp.stack([q_base // BK, q_base // BM, (jnp.max(lim.reshape(-1, BQ), axis=1) + BM - 1) // BM]).astype(jnp.int32)
        lim_w = jnp.broadcast_to(lim[:, None], (2 * seq_loc, 128))
        flag_w = jnp.broadcast_to(is_img[:, None], (2 * seq_loc, 128))
        inv_freq = ROPE_BASE ** (-jnp.arange(0, HEAD, 2).astype(F32) / HEAD)
        angle = (pos.astype(F32) / ROPE_SCALE)[:, None] * inv_freq[None, :]
        cos_t, sin_t = jnp.cos(angle), jnp.sin(angle)

        pooled_own = pool_patches(vis_loc)
        pooled_mate = swap_x(pooled_own)
        text_src, _ = lax.optimization_barrier((text_loc, pooled_mate))
        text_mate = swap_x(text_src)
        dy_src, _ = lax.optimization_barrier((grad_y, text_mate))
        dy_mate = swap_x(dy_src)
        n_own = pooled_own.shape[0]
        pooled = jnp.where(is_lo, jnp.concatenate([pooled_own, pooled_mate]), jnp.concatenate([pooled_mate, pooled_own]))
        normed, norm_pull = jax.vjp(gain_norm, pooled, pn_gain.astype(F32))
        soft = dot(normed, w_proj).astype(BF16)
        soft_all = jnp.concatenate([soft, swap_c(soft)])

        x, hidden, q_raw, q, k_raw, k, v = qkv_call(meta, text_loc, text_mate, soft_all, pre1, w_query, w_key, w_value, qg1, kg1, cos_t, sin_t)

        def by_position(mine, theirs):
            a = jnp.where(first, mine, theirs)
            b = jnp.where(first, theirs, mine)
            return jnp.concatenate([a[:seq_loc], b, a[seq_loc:]])

        kv = jnp.concatenate([k, v], axis=1)
        kv_all = by_position(kv, swap_c(kv))
        k_all, v_all = kv_all[:, :HEAD], kv_all[:, HEAD:]
        kt_all = k_all.T
        hidden_c = swap_c(hidden)
        o, lse = fwd_call(span, q, kt_all, v_all, lim_w)
        y_loc, d_a, d_o, delta, g_post = out_call(meta, o, x, grad_y, dy_mate, w_out, post1)
        cols = w_query.shape[1] // 2
        pick_cols = lambda v, flag: jnp.where(flag, v[:, :cols], v[:, cols:])
        o_c = swap_c(pick_cols(o, ~first))
        d_a_c = swap_c(d_a)
        delta_t = delta.T[:, None, :]
        dq_raw, g_qg, dk_part, dv_part = bwd_call(span, q, d_o, k_all, kt_all, v_all, lim[None], lse, delta_t, q_raw, qg1, cos_t, sin_t)
        g_out_half = (tdot(pick_cols(o, first), d_a) + tdot(o_c, d_a_c)).astype(BF16)
        g_out_other = swap_c(g_out_half)
        g_out = jnp.where(first, jnp.concatenate([g_out_half, g_out_other]), jnp.concatenate([g_out_other, g_out_half]))

        dkv_part = jnp.concatenate([dk_part, dv_part], axis=1)
        set_a = jnp.concatenate([dkv_part[:seq_loc], dkv_part[3 * seq_loc:]])
        set_b = dkv_part[seq_loc:3 * seq_loc]
        dkv_c = swap_c(jnp.where(first, set_b, set_a))
        grad_text, d_merged, dk_raw, d_v, g_pre, g_kg = hid_call(
            meta, dq_raw, dk_part, dv_part, dkv_c, k_raw, cos_t, sin_t, kg1, w_query, w_key, w_value, x, pre1, grad_y, dy_mate, flag_w)

        d_merged_c = swap_c(d_merged)
        my_img = jnp.concatenate([2 * lo_dev + jnp.arange(2), 2 * hi_dev + jnp.arange(2)])
        start = img_pos[my_img]
        blk0 = start // RB
        blk1 = jnp.minimum(blk0 + 1, seq // RB - 1)

        def locate(g):
            owner = g // half
            in_set = jnp.minimum(owner, n_dev - 1 - owner)
            return g % half + jnp.where(owner >= n_dev // 2, half, 0), (in_set == my_set).astype(jnp.int32)

        at0, mine0 = locate(blk0)
        at1, mine1 = locate(blk1)
        d_soft = pick_call(jnp.stack([at0, at1, start % RB, mine0, mine1]).astype(jnp.int32), d_merged, d_merged_c)
        d_normed = dot_t(d_soft, w_proj).astype(BF16)
        d_pooled, g_pn = norm_pull(d_normed)
        d_own = jnp.where(is_lo, d_pooled[:n_own], d_pooled[n_own:])
        grad_vis = unpool_grad(d_own, vis_loc.shape[0])
        g_proj_part = tdot(normed, d_soft)
        pc = g_proj_part.shape[0] // 2
        p_lo, p_hi = g_proj_part[:pc], g_proj_part[pc:]
        g_proj_half = (jnp.where(first, p_lo, p_hi) + swap_c(jnp.where(first, p_hi, p_lo))).astype(BF16)
        g_proj_other = swap_c(g_proj_half)
        g_proj = jnp.where(first, jnp.concatenate([g_proj_half, g_proj_other]), jnp.concatenate([g_proj_other, g_proj_half]))

        mine = jnp.concatenate([pick_cols(dq_raw, first), jnp.where(first, dk_raw, d_v)], axis=1)
        dq_c = swap_c(pick_cols(dq_raw, ~first))
        kv_c = swap_c(jnp.where(first, d_v, dk_raw))
        theirs = jnp.concatenate([dq_c, kv_c], axis=1)
        g_half = (tdot(hidden, mine) + tdot(hidden_c, theirs)).astype(BF16)
        g_other = swap_c(g_half)
        g_a = jnp.where(first, g_half, g_other)
        g_b = jnp.where(first, g_other, g_half)
        g_query = jnp.concatenate([g_a[:, :cols], g_b[:, :cols]], axis=1)
        g_key, g_value = g_a[:, cols:], g_b[:, cols:]

        small = jnp.concatenate([g_pn, g_pre[0], g_qg[0], g_kg[0], g_post[0]])
        small = (small + swap_c(small)).astype(BF16)
        cuts = [g_pn.shape[0]]
        for g in (g_pre, g_qg, g_kg):
            cuts.append(cuts[-1] + g.shape[1])
        g_pn, g_pre, g_qg, g_kg, g_post = jnp.split(small, cuts)
        return (y_loc, grad_text, grad_vis, g_pn, g_proj, g_pre, g_query, g_key, g_value, g_qg, g_kg, g_out, g_post)

    in_specs = (seq_spec, seq_spec, part_spec, seq_spec) + (rep_spec,) * 10
    out_specs = (seq_spec, seq_spec, seq_spec) + (part_spec,) * 10
    return jax.shard_map(device_body, mesh=mesh, in_specs=in_specs, out_specs=out_specs, check_vma=False)
```

```python
import functools
import jax
import jax.numpy as jnp
from jax import lax
from jax.experimental import pallas as pl
from jax.experimental.pallas import tpu as pltpu
from jax.sharding import PartitionSpec as P

GRID = 64
POOL = 4
SIDE = GRID // POOL
BLOCK = SIDE * SIDE
EPS = 1e-6
ROPE_BASE = 1000000.0
ROPE_SCALE = 8.0
NEG_BIG = -1e30
HEAD = 256
HALF = HEAD // 2
BF = 256
RB = 256
VMEM_LIMIT = 60 * 1024 * 1024
F32 = jnp.float32
ZERO = 0
ALL = Ellipsis
BF16 = jnp.bfloat16


def params(sem):
    return pltpu.CompilerParams(dimension_semantics=sem, vmem_limit_bytes=VMEM_LIMIT)


def cost(flops, nbytes):
    return pl.CostEstimate(flops=int(flops), bytes_accessed=int(nbytes), transcendentals=0)


def dot(a, b):
    return jnp.dot(a, b, preferred_element_type=F32)


def dot_t(a, b):
    return lax.dot_general(a, b, (((1,), (1,)), ((), ())), preferred_element_type=F32)


def col_sum(v):
    return jnp.sum(v, axis=0, keepdims=True)


def row_mean(v):
    return jnp.mean(v, axis=-1, keepdims=True)


def iota(shape, axis):
    return lax.broadcasted_iota(jnp.int32, shape, axis)


def pool_kernel(vis_ref, out_ref):
    rows, cols = SIDE, POOL * GRID
    patch = iota((rows, cols), 1) % GRID
    sel = (patch // POOL == iota((rows, cols), 0)).astype(BF16)
    for i in range(vis_ref.shape[1] // cols):
        total = dot(sel, vis_ref[0, i * cols:(i + 1) * cols, :])
        out_ref[i * rows:(i + 1) * rows, :] = (total / (POOL * POOL)).astype(BF16)


def pool_patches(vis_loc):
    n_img, n_patch, dim = vis_loc.shape
    bands = 4
    steps = SIDE // bands
    return pl.pallas_call(
        pool_kernel,
        out_shape=jax.ShapeDtypeStruct((n_img * BLOCK, dim), BF16),
        grid=(n_img, steps),
        in_specs=[pl.BlockSpec((1, bands * POOL * GRID, dim), lambda n, i: (n, i, 0))],
        out_specs=pl.BlockSpec((bands * SIDE, dim), lambda n, i: (n * steps + i, 0)),
        compiler_params=params(("arbitrary", "arbitrary")),
        cost_estimate=cost(4e9, n_img * n_patch * dim * 2),
        name="pool",
    )(vis_loc)


def unpool_kernel(d_ref, out_ref):
    sel = (iota((GRID, SIDE), 0) // POOL == iota((GRID, SIDE), 1)).astype(BF16)
    for i in range(out_ref.shape[1] // (POOL * GRID)):
        band = (d_ref[i * SIDE:(i + 1) * SIDE, :].astype(F32) / (POOL * POOL)).astype(BF16)
        line = dot(sel, band).astype(BF16)
        for j in range(POOL):
            at = (i * POOL + j) * GRID
            out_ref[0, at:at + GRID, :] = line


def unpool_grad(d_pooled, n_img):
    dim = d_pooled.shape[1]
    bands = 4
    steps = SIDE // bands
    return pl.pallas_call(
        unpool_kernel,
        out_shape=jax.ShapeDtypeStruct((n_img, GRID * GRID, dim), BF16),
        grid=(n_img, steps),
        in_specs=[pl.BlockSpec((bands * SIDE, dim), lambda n, i: (n * steps + i, 0))],
        out_specs=pl.BlockSpec((1, bands * POOL * GRID, dim), lambda n, i: (n, i, 0)),
        compiler_params=params(("arbitrary", "arbitrary")),
        cost_estimate=cost(4e9, n_img * GRID * GRID * dim * 2),
        name="unpool",
    )(d_pooled)


def rms(x):
    return lax.rsqrt(row_mean(x * x) + EPS)


def norm_rope(raw, gain1, cos_t, sin_t):
    x = raw.astype(F32)
    x = x * rms(x) * gain1
    lo, hi = x[:, :HALF], x[:, HALF:]
    return (lo * cos_t - hi * sin_t).astype(BF16), (hi * cos_t + lo * sin_t).astype(BF16)


def norm_rope_grad(d_out, raw, gain1, cos_t, sin_t):
    d = d_out.astype(F32)
    lo, hi = d[:, :HALF], d[:, HALF:]
    d = jnp.concatenate([lo * cos_t + hi * sin_t, hi * cos_t - lo * sin_t], axis=1)
    x = raw.astype(F32)
    r = rms(x)
    xr = x * r
    dg = d * gain1
    d_raw = r * (dg - xr * row_mean(xr * dg))
    return d_raw.astype(BF16), col_sum(d * xr)


def qkv_kernel(n_text, meta, *refs):
    texts, refs = refs[:n_text], refs[n_text:]
    softs, refs = refs[:4], refs[4:]
    pre1, wq, wk, wv, qg1, kg1, cos_ref, sin_ref = refs[:8]
    x_out, hid_out, qraw_out, q_out, kraw_out, kv_out, x_scr = refs[-7:]
    i = pl.program_id(0)
    c = meta[0, 0] + i if n_text == 1 else meta[0, 1] + i
    if n_text == 1:
        x_scr[ALL] = texts[0][ALL]
    else:
        @pl.when(i == 0)
        def _():
            x_scr[ALL] = texts[0][ALL]

        @pl.when(i > 0)
        def _():
            x_scr[ALL] = texts[1][ALL]

    for slot in (0, 1):
        off = meta[2 + 3 * slot, c]
        for kind in (0, 1):
            soft = softs[2 * slot + kind]

            @pl.when((off < RB) & (meta[3 + 3 * slot, c] == kind))
            def _():
                src = iota((RB, BLOCK), 0) - off
                pick = (src == iota((RB, BLOCK), 1)).astype(BF16)
                row = iota((RB, 1), 0) - off
                inside = (row >= 0) & (row < BLOCK)
                x_scr[ALL] = jnp.where(inside, dot(pick, soft[ALL]).astype(BF16), x_scr[ALL])

    x_out[ALL] = x_scr[ALL]
    x = x_scr[ALL].astype(F32)
    hid_out[ALL] = (x * rms(x) * pre1[ALL]).astype(BF16)
    hid = hid_out[ALL]
    kraw_out[ALL] = dot(hid, wk[ALL]).astype(BF16)
    kv_out[:, HEAD:] = dot(hid, wv[ALL]).astype(BF16)
    cos_t, sin_t = cos_ref[ALL], sin_ref[ALL]
    lo, hi = norm_rope(kraw_out[ALL], kg1[ALL], cos_t, sin_t)
    kv_out[:, :HALF] = lo
    kv_out[:, HALF:HEAD] = hi
    for h in range(q_out.shape[1] // HEAD):
        raw = dot(hid, wq[:, h * HEAD:(h + 1) * HEAD]).astype(BF16)
        qraw_out[:, h * HEAD:(h + 1) * HEAD] = raw
        lo, hi = norm_rope(raw, qg1[ALL], cos_t, sin_t)
        q_out[:, h * HEAD:h * HEAD + HALF] = (lo * 0.0625).astype(BF16)
        q_out[:, h * HEAD + HALF:(h + 1) * HEAD] = (hi * 0.0625).astype(BF16)


def qkv_call(meta, texts, softs, pre1, wq, wk, wv, qg1, kg1, cos_t, sin_t, prev=()):
    rows = sum(t.shape[0] for t in texts)
    dim = texts[0].shape[1]
    steps = rows // RB
    width = wq.shape[1]
    side = 0 if len(texts) == 1 else 1

    def row(w):
        return pl.BlockSpec((RB, w), lambda i, meta: (meta[0, side] + i, 0))

    def whole(a):
        return pl.BlockSpec(a.shape, lambda i, meta: (0,) * a.ndim, pipeline_mode=pl.Buffered(1))

    def soft_spec(slot, kind):
        def index(i, meta):
            c = meta[0, side] + i
            return jnp.where(meta[3 + 3 * slot, c] == kind, meta[1 + 3 * slot, c], 0), 0

        return pl.BlockSpec((BLOCK, dim), index)

    def struct(w):
        return jax.ShapeDtypeStruct((2 * rows, w), BF16)

    if side == 0:
        text_specs = [pl.BlockSpec((RB, dim), lambda i, meta: (i, ZERO))]
    else:
        text_specs = [pl.BlockSpec((RB, dim), lambda i, meta: (ZERO, ZERO)),
                      pl.BlockSpec((RB, dim), lambda i, meta: (jnp.maximum(i - 1, 0), 0))]
    n_in = 1 + len(texts) + 4 + 8
    return pl.pallas_call(
        functools.partial(qkv_kernel, len(texts)),
        out_shape=[struct(dim), struct(dim), struct(width), struct(width), struct(HEAD), struct(2 * HEAD)],
        grid_spec=pltpu.PrefetchScalarGridSpec(
            num_scalar_prefetch=1, grid=(steps,),
            in_specs=text_specs + [soft_spec(ZERO, ZERO), soft_spec(0, 1), soft_spec(1, 0), soft_spec(1, 1)]
            + [whole(pre1), whole(wq), whole(wk), whole(wv), whole(qg1), whole(kg1), row(HALF), row(HALF)]
            + [pl.BlockSpec(memory_space=pl.ANY)] * len(prev),
            out_specs=[row(dim), row(dim), row(width), row(width), row(HEAD), row(2 * HEAD)],
            scratch_shapes=[pltpu.VMEM((RB, dim), BF16)]),
        input_output_aliases={n_in + k: k for k in range(len(prev))},
        compiler_params=params(("arbitrary",)),
        cost_estimate=cost(2 * rows * dim * (width + 2 * HEAD), 30e6),
        name="qkv",
    )(meta, *texts, softs[0], softs[1], softs[0], softs[1], pre1, wq, wk, wv, qg1, kg1, cos_t, sin_t, *prev)


def arrange_kernel(meta, mine, theirs, k_ref, v_ref, kt_ref, vt_ref):
    i = pl.program_id(0)

    def put(kv):
        k_ref[ALL] = kv[:, :HEAD]
        v_ref[ALL] = kv[:, HEAD:]
        kt_ref[ALL] = kv[:, :HEAD].astype(F32).T.astype(BF16)
        vt_ref[ALL] = kv[:, HEAD:].astype(F32).T.astype(BF16)

    @pl.when(meta[1, i] == 1)
    def _():
        put(mine[ALL])

    @pl.when(meta[1, i] == 0)
    def _():
        put(theirs[ALL])


def arrange_call(meta, mine, theirs):
    seq = 2 * mine.shape[0]
    blocks = meta.shape[1]
    rows = seq // blocks
    spec = lambda flag: pl.BlockSpec((rows, 2 * HEAD), lambda i, m: (jnp.where(m[1, i] == flag, m[0, i], 0), 0))
    tall = pl.BlockSpec((rows, HEAD), lambda i, m: (i, ZERO))
    flat = pl.BlockSpec((HEAD, rows), lambda i, m: (0, i))
    return pl.pallas_call(
        arrange_kernel,
        out_shape=[jax.ShapeDtypeStruct((seq, HEAD), BF16)] * 2 + [jax.ShapeDtypeStruct((HEAD, seq), BF16)] * 2,
        grid_spec=pltpu.PrefetchScalarGridSpec(
            num_scalar_prefetch=1, grid=(blocks,), in_specs=[spec(1), spec(0)], out_specs=[tall, tall, flat, flat]),
        compiler_params=params(("arbitrary",)),
        cost_estimate=cost(1e9, 12e6),
        name="arrange",
    )(meta, mine, theirs)


def fwd_kernel(span, q_ref, k_ref, vt_ref, lim_ref, o_ref, lse_ref, qt, acc, m_scr, l_scr):
    b = pl.program_id(0)
    heads = qt.shape[0]
    rows = q_ref.shape[0]
    for h in range(heads):
        qt[h] = q_ref[:, h * HEAD:(h + 1) * HEAD].astype(F32).T.astype(BF16)
    acc[ALL] = jnp.zeros_like(acc)
    m_scr[ALL] = jnp.full_like(m_scr, NEG_BIG)
    l_scr[ALL] = jnp.zeros_like(l_scr)

    def step(j, bk, masked):
        off = pl.multiple_of(j * bk, bk)
        keys = k_ref[pl.ds(off, bk), :]
        vals = vt_ref[:, pl.ds(off, bk)]
        if masked:
            seen = off + iota((bk, rows), 0) < lim_ref[ALL]
        for h in range(heads):
            s = dot(keys, qt[h])
            if masked:
                s = jnp.where(seen, s, NEG_BIG)
            m_old = m_scr[h]
            m_new = jnp.maximum(m_old, jnp.max(s, axis=0, keepdims=True))
            p = jnp.exp(s - m_new)
            alpha = jnp.exp(m_old - m_new)
            l_scr[h] = alpha * l_scr[h] + col_sum(p)
            m_scr[h] = m_new
            acc[h] = acc[h] * alpha + dot(vals, p.astype(BF16))

    @pl.loop(0, span[0, b])
    def _(j):
        step(j, 4 * BF, False)

    @pl.loop(span[1, b], span[2, b])
    def _(j):
        step(j, 2 * BF, False)

    @pl.loop(span[3, b], span[4, b])
    def _(j):
        step(j, BF, True)

    for h in range(heads):
        o_ref[:, h * HEAD:(h + 1) * HEAD] = (acc[h] / l_scr[h]).T.astype(BF16)
        lse_ref[h] = m_scr[h] + jnp.log(l_scr[h])


def fwd_call(span, q, k, vt, lim):
    rows, width = q.shape
    heads = width // HEAD
    seq = k.shape[0]
    wide = pl.BlockSpec((BF, width), lambda b, s: (b, 0))
    return pl.pallas_call(
        fwd_kernel,
        out_shape=[jax.ShapeDtypeStruct((rows, width), BF16), jax.ShapeDtypeStruct((heads, 1, rows), F32)],
        grid_spec=pltpu.PrefetchScalarGridSpec(
            num_scalar_prefetch=1, grid=(rows // BF,),
            in_specs=[wide, pl.BlockSpec((seq, HEAD), lambda b, s: (ZERO, ZERO)), pl.BlockSpec((HEAD, seq), lambda b, s: (ZERO, ZERO)),
                      pl.BlockSpec((1, BF), lambda b, s: (ZERO, b))],
            out_specs=[wide, pl.BlockSpec((heads, 1, BF), lambda b, s: (0, 0, b))],
            scratch_shapes=[pltpu.VMEM((heads, HEAD, BF), BF16), pltpu.VMEM((heads, HEAD, BF), F32),
                            pltpu.VMEM((heads, 1, BF), F32), pltpu.VMEM((heads, 1, BF), F32)]),
        compiler_params=params(("arbitrary",)),
        cost_estimate=cost(2 * rows * seq * width, 30e6),
        name="attn_fwd",
    )(span, q, k, vt, lim)


def bwd_kernel(span, q_ref, do_ref, k_ref, kt_ref, v_ref, lim_ref, lse_ref, delta_ref, qraw_ref, qg1, cos_ref, sin_ref,
               dq_mine, dq_theirs, gq_ref, dkv_mine, dkv_theirs, qt, dot_scr, dqt, dk_scr, dv_scr):
    b, h = pl.program_id(0), pl.program_id(1)
    heads = pl.num_programs(1)
    bq = q_ref.shape[0]
    mid = bq // 2

    @pl.when((b == 0) & (h == 0))
    def _():
        dk_scr[ALL] = jnp.zeros_like(dk_scr)
        dv_scr[ALL] = jnp.zeros_like(dv_scr)
        gq_ref[ALL] = jnp.zeros_like(gq_ref)

    qt[ALL] = q_ref[ALL].astype(F32).T.astype(BF16)
    dot_scr[ALL] = do_ref[ALL].astype(F32).T.astype(BF16)
    dqt[ALL] = jnp.zeros_like(dqt)

    def step(off, bk, masked, lo, hi):
        off = pl.multiple_of(off, bk)
        rows = pl.ds(off, bk)
        c = slice(lo, hi)
        p = jnp.exp(dot(k_ref[rows, :], qt[:, c]) - lse_ref[0][:, c])
        if masked:
            p = jnp.where(off + iota(p.shape, 0) < lim_ref[:, c], p, 0.0)
        ds = (p * (dot(v_ref[rows, :], dot_scr[:, c]) - delta_ref[0][:, c])).astype(BF16)
        dv_scr[rows, :] += dot(p.astype(BF16), do_ref[c, :])
        dk_scr[rows, :] += dot(ds, q_ref[c, :])
        dqt[:, c] += dot(kt_ref[:, rows], ds)

    base = span[0, b] * mid

    @pl.loop(0, span[0, b])
    def _(j):
        step(j * mid, mid, False, 0, bq)

    step(base, mid, True, 0, bq)
    step(base + mid, mid, True, mid, bq)

    @pl.when(span[1, b] == 1)
    def _():
        step(base + mid, BLOCK, True, mid - BLOCK, mid)

    @pl.when(span[2, b] == 1)
    def _():
        step(base + bq, BLOCK, True, bq - BLOCK, bq)

    d_q = (dqt[ALL].T * 0.0625).astype(BF16)
    d_raw, g_part = norm_rope_grad(d_q, qraw_ref[ALL], qg1[ALL], cos_ref[ALL], sin_ref[ALL])
    gq_ref[ALL] += g_part

    @pl.when(h < heads // 2)
    def _():
        dq_mine[ALL] = d_raw

    @pl.when(h >= heads // 2)
    def _():
        dq_theirs[ALL] = d_raw

    @pl.when((b == pl.num_programs(0) - 1) & (h == heads - 1))
    def _():
        for kind, out in ((0, dkv_mine), (1, dkv_theirs)):
            for part in (0, 1):
                src = pl.ds(pl.multiple_of(span[3 + kind, part] * bq, bq), bq)
                dst = slice(part * bq, (part + 1) * bq)
                out[dst, :HEAD] = dk_scr[src, :]
                out[dst, HEAD:] = dv_scr[src, :]


def bwd_call(span, q, d_o, k, kt, v, lim, lse, delta, q_raw, qg1, cos_t, sin_t):
    rows, width = q.shape
    heads = width // HEAD
    seq = v.shape[0]
    bq = rows // 2
    head = lambda h, s: (h + s[5, 0]) % heads
    tile = pl.BlockSpec((bq, HEAD), lambda b, h, s: (b, head(h, s)))
    fixed = lambda shape: pl.BlockSpec(shape, lambda b, h, s: (ZERO, ZERO))
    keys = pl.BlockSpec((seq, HEAD), lambda b, h, s: (ZERO, ZERO), pipeline_mode=pl.Buffered(1))
    stat = pl.BlockSpec((1, 1, bq), lambda b, h, s: (head(h, s), 0, b))
    rot = pl.BlockSpec((bq, HALF), lambda b, h, s: (b, 0))
    struct = jax.ShapeDtypeStruct
    return pl.pallas_call(
        bwd_kernel,
        out_shape=[struct((rows, width // 2), BF16), struct((rows, width // 2), BF16), struct((1, HEAD), F32),
                   struct((rows, 2 * HEAD), F32), struct((rows, 2 * HEAD), F32)],
        grid_spec=pltpu.PrefetchScalarGridSpec(
            num_scalar_prefetch=1, grid=(2, heads),
            in_specs=[tile, tile, keys, pl.BlockSpec((HEAD, seq), lambda b, h, s: (ZERO, ZERO), pipeline_mode=pl.Buffered(1)), keys,
                      pl.BlockSpec((1, bq), lambda b, h, s: (ZERO, b)), stat, stat, tile, fixed((1, HEAD)), rot, rot],
            out_specs=[pl.BlockSpec((bq, HEAD), lambda b, h, s: (b, jnp.minimum(h, heads // 2 - 1))),
                       pl.BlockSpec((bq, HEAD), lambda b, h, s: (b, jnp.maximum(h - heads // 2, 0))),
                       fixed((1, HEAD)), fixed((rows, 2 * HEAD)), fixed((rows, 2 * HEAD))],
            scratch_shapes=[pltpu.VMEM((HEAD, bq), BF16), pltpu.VMEM((HEAD, bq), BF16), pltpu.VMEM((HEAD, bq), F32),
                            pltpu.VMEM((seq, HEAD), F32), pltpu.VMEM((seq, HEAD), F32)]),
        compiler_params=params(("arbitrary", "arbitrary")),
        cost_estimate=cost(5 * rows * seq * width, 50e6),
        name="attn_bwd",
    )(span, q, d_o, k, kt, v, lim, lse, delta, q_raw, qg1, cos_t, sin_t)


def out_kernel(meta, o_ref, x_ref, dy_own, dy_mate, wo, post1,
               y_ref, da_ref, do_ref, delta_ref, gpost_ref, o_mine, o_theirs):
    i = pl.program_id(0)
    half = pl.num_programs(0) // 2
    own = (i < half) == (meta[0, 0] == 0)
    parts = [slice(k * RB, (k + 1) * RB) for k in range(o_ref.shape[0] // RB)]
    a_all = [dot(o_ref[c, :], wo[ALL]).astype(BF16) for c in parts]
    g_post = jnp.where(i == 0, jnp.zeros_like(gpost_ref[ALL]), gpost_ref[ALL])
    for c, a_lo in zip(parts, a_all):
        a = a_lo.astype(F32)
        ar = a * rms(a)
        y = x_ref[c, :].astype(F32) + ar * post1[ALL]

        @pl.when(own)
        def _():
            y_ref[c, :] = y.astype(BF16)

    for c, a_lo in zip(parts, a_all):
        a = a_lo.astype(F32)
        r = rms(a)
        ar = a * r
        dy = jnp.where(own, dy_own[c, :], dy_mate[c, :]).astype(F32)
        g_post = g_post + col_sum(dy * ar)
        dg = dy * post1[ALL]
        da_ref[c, :] = (r * (dg - ar * row_mean(ar * dg))).astype(BF16)
        do_ref[c, :] = dot_t(da_ref[c, :], wo[ALL]).astype(BF16)
        cols = []
        for h in range(o_ref.shape[1] // HEAD):
            d = slice(h * HEAD, (h + 1) * HEAD)
            cols.append(jnp.sum(do_ref[c, d].astype(F32) * o_ref[c, d].astype(F32), axis=-1, keepdims=True))
        delta_ref[c, :] = jnp.concatenate(cols, axis=1)
    gpost_ref[ALL] = g_post
    for kind, out in enumerate((o_mine, o_theirs)):
        width = out.shape[1]
        at = pl.multiple_of(((meta[0, 2] ^ kind) * 2 + meta[0, 3]) * width, width)
        out[ALL] = o_ref[:, pl.ds(at, width)]


def split_cols(first, src, mine, theirs):
    cut = src.shape[1] // 2

    @pl.when(first)
    def _():
        mine[ALL] = src[:, :cut]
        theirs[ALL] = src[:, cut:]

    @pl.when(jnp.logical_not(first))
    def _():
        mine[ALL] = src[:, cut:]
        theirs[ALL] = src[:, :cut]


def own_maps(half):
    def own_map(i, meta):
        is_lo = meta[0, 0] == 0
        return jnp.where(is_lo, jnp.minimum(i, half - 1), jnp.maximum(i - half, 0)), 0

    def mate_map(i, meta):
        is_lo = meta[0, 0] == 0
        return jnp.where(is_lo, jnp.maximum(i - half, 0), jnp.minimum(i, half - 1)), 0

    return own_map, mate_map


def out_call(meta, o, x, dy_own, dy_mate, wo, post1):
    rows, width = o.shape
    dim = wo.shape[1]
    step = 2 * RB
    steps = rows // step
    own_map, mate_map = own_maps(steps // 2)
    row = lambda w: pl.BlockSpec((step, w), lambda i, meta: (i, ZERO))
    gain = pl.BlockSpec((1, dim), lambda i, meta: (ZERO, ZERO))
    struct = lambda w: jax.ShapeDtypeStruct((rows, w), BF16)
    heads = width // HEAD
    return pl.pallas_call(
        out_kernel,
        out_shape=[jax.ShapeDtypeStruct(dy_own.shape, BF16), struct(dim), struct(width),
                   jax.ShapeDtypeStruct((rows, heads), F32), jax.ShapeDtypeStruct((1, dim), F32),
                   struct(width // 4), struct(width // 4)],
        grid_spec=pltpu.PrefetchScalarGridSpec(
            num_scalar_prefetch=1, grid=(steps,),
            in_specs=[row(width), row(dim), pl.BlockSpec((step, dim), own_map), pl.BlockSpec((step, dim), mate_map),
                      pl.BlockSpec(wo.shape, lambda i, meta: (ZERO, ZERO), pipeline_mode=pl.Buffered(1)), gain],
            out_specs=[pl.BlockSpec((step, dim), own_map), row(dim), row(width), row(heads), gain,
                       row(width // 4), row(width // 4)]),
        compiler_params=params(("arbitrary",)),
        cost_estimate=cost(4 * rows * dim * width, 60e6),
        name="out_proj",
    )(meta, o, x, dy_own, dy_mate, wo, post1)


def hid_kernel(meta, dq_mine, dq_theirs, dkv_mine, dkv_theirs, kraw_ref, cos_ref, sin_ref, kg1, wq_mine, wq_theirs, wk, wv, x_ref,
               pre1, dy_own, dy_mate, lim_ref, dtext_ref, dm_ref, dk_ref, dv_ref, gpre_ref, gk_ref):
    i = pl.program_id(0)
    half = pl.num_programs(0) // 2
    own = (i < half) == (meta[0, 0] == 0)
    g_pre = jnp.where(i == 0, jnp.zeros_like(gpre_ref[ALL]), gpre_ref[ALL])
    g_k = jnp.where(i == 0, jnp.zeros_like(gk_ref[ALL]), gk_ref[ALL])
    d_k = (dkv_mine[:, :HEAD] + dkv_theirs[:, :HEAD]).astype(BF16)
    dv_ref[ALL] = (dkv_mine[:, HEAD:] + dkv_theirs[:, HEAD:]).astype(BF16)
    dk_ref[ALL], g_part = norm_rope_grad(d_k, kraw_ref[ALL], kg1[ALL], cos_ref[ALL], sin_ref[ALL])
    gk_ref[ALL] = g_k + g_part
    parts = [slice(k * RB, (k + 1) * RB) for k in range(x_ref.shape[0] // RB)]
    dh_all = []
    for c in parts:
        dh = dot_t(dq_mine[c, :], wq_mine[ALL]) + dot_t(dq_theirs[c, :], wq_theirs[ALL])
        dh = dh + dot_t(dk_ref[c, :], wk[ALL]) + dot_t(dv_ref[c, :], wv[ALL])
        dh_all.append(dh.astype(BF16))
    for c, dh in zip(parts, dh_all):
        dh = dh.astype(F32)
        x = x_ref[c, :].astype(F32)
        r = rms(x)
        xr = x * r
        g_pre = g_pre + col_sum(dh * xr)
        dg = dh * pre1[ALL]
        dx = (r * (dg - xr * row_mean(xr * dg))).astype(BF16).astype(F32)
        dm_ref[c, :] = (jnp.where(own, dy_own[c, :], dy_mate[c, :]).astype(F32) + dx).astype(BF16)
    gpre_ref[ALL] = g_pre

    @pl.when(own)
    def _():
        dtext_ref[ALL] = jnp.where(lim_ref[:, :1] > 0, jnp.zeros_like(dm_ref[ALL]), dm_ref[ALL])


def hid_call(meta, dq_mine, dq_theirs, dkv_mine, dkv_theirs, k_raw, cos_t, sin_t, kg1, wq, wk, wv, x, pre1, dy_own, dy_mate, img_flag):
    rows = x.shape[0]
    dim, width = wq.shape
    cut = width // 2
    step = 2 * RB
    steps = rows // step
    own_map, mate_map = own_maps(steps // 2)
    row = lambda w: pl.BlockSpec((step, w), lambda i, meta: (i, ZERO))
    half_w = lambda flip: pl.BlockSpec((dim, cut), lambda i, meta: (0, meta[0, 2] ^ flip), pipeline_mode=pl.Buffered(1))
    whole = lambda a: pl.BlockSpec(a.shape, lambda i, meta: (ZERO, ZERO), pipeline_mode=pl.Buffered(1))
    return pl.pallas_call(
        hid_kernel,
        out_shape=[jax.ShapeDtypeStruct(dy_own.shape, BF16), jax.ShapeDtypeStruct((rows, dim), BF16),
                   jax.ShapeDtypeStruct((rows, HEAD), BF16), jax.ShapeDtypeStruct((rows, HEAD), BF16),
                   jax.ShapeDtypeStruct((1, dim), F32), jax.ShapeDtypeStruct((1, HEAD), F32)],
        grid_spec=pltpu.PrefetchScalarGridSpec(
            num_scalar_prefetch=1, grid=(steps,),
            in_specs=[row(cut), row(cut), row(2 * HEAD), row(2 * HEAD), row(HEAD), row(HALF), row(HALF), whole(kg1),
                      half_w(0), half_w(1), whole(wk), whole(wv), row(dim), whole(pre1),
                      pl.BlockSpec((step, dim), own_map), pl.BlockSpec((step, dim), mate_map), row(128)],
            out_specs=[pl.BlockSpec((step, dim), own_map), row(dim), row(HEAD), row(HEAD),
                       pl.BlockSpec((1, dim), lambda i, meta: (ZERO, ZERO)), pl.BlockSpec((1, HEAD), lambda i, meta: (ZERO, ZERO))]),
        compiler_params=params(("arbitrary",)),
        cost_estimate=cost(2 * rows * dim * (width + 2 * HEAD), 60e6),
        name="hid_bwd",
    )(meta, dq_mine, dq_theirs, dkv_mine, dkv_theirs, k_raw, cos_t, sin_t, kg1, wq, wq, wk, wv, x, pre1, dy_own, dy_mate, img_flag)


def pick_kernel(meta, mine0, theirs0, mine1, theirs1, out_ref, out_mine, out_theirs, blk):
    n = pl.program_id(0)
    off = meta[2, n]
    for slot, mine, theirs in ((0, mine0, theirs0), (1, mine1, theirs1)):
        is_mine = meta[3 + slot, n] == 1

        @pl.when(is_mine)
        def _():
            blk[ALL] = mine[ALL]

        @pl.when(jnp.logical_not(is_mine))
        def _():
            blk[ALL] = theirs[ALL]

        src = iota((BLOCK, RB), 0) + off - slot * RB
        pick = (src == iota((BLOCK, RB), 1)).astype(BF16)
        if slot == 0:
            out_ref[ALL] = dot(pick, blk[ALL]).astype(BF16)
        else:
            out_ref[ALL] = jnp.where(src[:, :1] >= 0, dot(pick, blk[ALL]).astype(BF16), out_ref[ALL])
    split_cols(meta[5, 0] == 0, out_ref, out_mine, out_theirs)


def pick_call(meta, mine, theirs):
    dim = mine.shape[1]
    n_img = meta.shape[1]
    at = lambda slot, kind: pl.BlockSpec((RB, dim), lambda n, meta: (jnp.where(meta[3 + slot, n] == kind, meta[slot, n], 0), 0))
    out = lambda w: pl.BlockSpec((BLOCK, w), lambda n, meta: (n, ZERO))
    struct = lambda w: jax.ShapeDtypeStruct((n_img * BLOCK, w), BF16)
    return pl.pallas_call(
        pick_kernel,
        out_shape=[struct(dim), struct(dim // 2), struct(dim // 2)],
        grid_spec=pltpu.PrefetchScalarGridSpec(
            num_scalar_prefetch=1, grid=(n_img,),
            in_specs=[at(0, 1), at(ZERO, ZERO), at(1, 1), at(1, 0)],
            out_specs=[out(dim), out(dim // 2), out(dim // 2)],
            scratch_shapes=[pltpu.VMEM((RB, dim), BF16)]),
        compiler_params=params(("arbitrary",)),
        cost_estimate=cost(4 * n_img * BLOCK * RB * dim, 20e6),
        name="pick_rows",
    )(meta, mine, theirs, mine, theirs)


def join_kernel(at_ref, *refs):
    pieces, out_ref = refs[:-1], refs[-1]
    for k, piece in enumerate(pieces):
        @pl.when(pl.program_id(0) == k)
        def _():
            out_ref[ALL] = piece[ALL]


def join_call(at, pieces, axis):
    rows, width = pieces[0].shape
    n = len(pieces)
    cuts = 2
    step = rows // cuts
    if axis == 0:
        shape = (n * rows, width)
        out = pl.BlockSpec((step, width), lambda h, i, at: (at[h] * cuts + i, 0))
    else:
        shape = (rows, n * width)
        out = pl.BlockSpec((step, width), lambda h, i, at: (i, at[h]))

    def spec(k):
        return pl.BlockSpec((step, width), lambda h, i, at: (jnp.where(h == k, i, jnp.where(h < k, 0, cuts - 1)), 0))

    return pl.pallas_call(
        join_kernel,
        out_shape=jax.ShapeDtypeStruct(shape, BF16),
        grid_spec=pltpu.PrefetchScalarGridSpec(
            num_scalar_prefetch=1, grid=(n, cuts), in_specs=[spec(k) for k in range(n)], out_specs=out),
        compiler_params=params(("arbitrary", "arbitrary")),
        cost_estimate=cost(1e9, 2 * n * rows * width * 2),
        name="join",
    )(at, *pieces)


def gain_norm(values, gain_vec):
    wide = values.astype(F32)
    return (wide * lax.rsqrt(row_mean(wide * wide) + EPS) * (1.0 + gain_vec)).astype(BF16)


def tdot(a, b):
    return lax.dot_general(a, b, (((0,), (0,)), ((), ())), preferred_element_type=F32)


def solution(mesh):
    n_dev = mesh.shape['cp']
    seq_spec = P(('dp', 'cp'))
    part_spec = P('dp')
    rep_spec = P()
    across = [(i, n_dev - 1 - i) for i in range(n_dev)]
    beside = [(i, i ^ 1) for i in range(n_dev)]

    def swap_x(v):
        return lax.ppermute(v, 'cp', across)

    def swap_c(v):
        return lax.ppermute(v, 'cp', beside)

    def device_body(vis_loc, text_loc, img_pos, grad_y, pn_gain, w_proj, pre_gain, w_query, w_key, w_value, q_gain, k_gain, w_out, post_gain):
        dev = lax.axis_index('cp')
        seq_loc, _ = text_loc.shape
        seq = seq_loc * n_dev
        mate = n_dev - 1 - dev
        lo_dev, hi_dev = jnp.minimum(dev, mate), jnp.maximum(dev, mate)
        is_lo = dev < mate
        chip = jnp.where(is_lo, 0, 1)
        my_set = lo_dev
        first = my_set == 0
        pre1 = (1.0 + pre_gain.astype(F32))[None]
        post1 = (1.0 + post_gain.astype(F32))[None]
        qg1 = (1.0 + q_gain.astype(F32))[None]
        kg1 = (1.0 + k_gain.astype(F32))[None]

        blocks = 2 * seq_loc // RB
        half = blocks // 2
        blk = jnp.arange(blocks)
        blk_base = jnp.where(blk < half, lo_dev * seq_loc + blk * RB, hi_dev * seq_loc + (blk - half) * RB)
        row = jnp.arange(2 * seq_loc)
        pos = jnp.where(row < seq_loc, lo_dev * seq_loc + row, (hi_dev - 1) * seq_loc + row)
        img = jnp.arange(img_pos.shape[0])
        img_dev = img // 2
        img_set = jnp.minimum(img_dev, n_dev - 1 - img_dev)
        img_slot = jnp.where(img_dev >= n_dev // 2, 2, 0) + img % 2
        img_kind = jnp.where(img_set == my_set, 0, 1)
        rel = img_pos[None, :] - blk_base[:, None]
        hit0 = (rel > -BLOCK) & (rel <= 0)
        hit1 = (rel > 0) & (rel < RB)
        of = lambda hit, v: jnp.sum(jnp.where(hit, v, 0), axis=1)
        off_of = lambda hit: jnp.where(jnp.any(hit, axis=1), of(hit, rel), seq)
        own_at = jnp.where(is_lo, 0, half)
        flags = jnp.where(blk == 0, own_at, jnp.where(blk == 1, half - own_at, jnp.where(blk == 2, my_set, chip)))
        meta = jnp.stack([flags, of(hit0, img_slot[None]), off_of(hit0), of(hit0, img_kind[None]),
                          of(hit1, img_slot[None]), off_of(hit1), of(hit1, img_kind[None])]).astype(jnp.int32)
        offset = pos[:, None] - img_pos[None, :]
        in_blk = (offset >= 0) & (offset < BLOCK)
        lim = jnp.maximum(pos + 1, jnp.max(jnp.where(in_blk, img_pos[None, :] + BLOCK, 0), axis=1)).astype(jnp.int32)
        is_img = jnp.any(in_blk, axis=1).astype(jnp.int32)
        f_end = jnp.max(lim.reshape(-1, BF), axis=1)
        f_base = blk_base if BF == RB else pos[::BF]
        f_span = jnp.stack([f_base // (4 * BF), f_base // (4 * BF) * 2, f_base // (2 * BF), f_base // (2 * BF) * 2,
                            (f_end + BF - 1) // BF]).astype(jnp.int32)
        half_end = jnp.max(lim.reshape(4, -1), axis=1)
        mid = seq_loc // 2
        mine_at = jnp.stack([lo_dev, hi_dev])
        their_at = jnp.stack([lo_dev ^ 1, hi_dev ^ 1])
        b_base = mine_at * seq_loc
        heads = w_query.shape[1] // HEAD
        b_span = jnp.stack([b_base // mid, half_end[0::2] > b_base + mid, half_end[1::2] > b_base + seq_loc, mine_at, their_at,
                            jnp.zeros_like(b_base) + my_set * (heads // 2)]).astype(jnp.int32)
        flag_w = jnp.broadcast_to(is_img[:, None], (2 * seq_loc, 128))
        dev_blk = jnp.arange(n_dev)
        kv_at = jnp.stack([jnp.where(dev_blk >= n_dev // 2, 1, 0),
                           jnp.minimum(dev_blk, n_dev - 1 - dev_blk) == my_set]).astype(jnp.int32)
        inv_freq = ROPE_BASE ** (-jnp.arange(0, HEAD, 2).astype(F32) / HEAD)
        angle = (pos.astype(F32) / ROPE_SCALE)[:, None] * inv_freq[None, :]
        cos_t, sin_t = jnp.cos(angle), jnp.sin(angle)
        halves_at = jnp.stack([my_set, 1 - my_set]).astype(jnp.int32)
        mine_q, their_q = 2 * my_set, 2 - 2 * my_set
        quarters_at = jnp.stack([mine_q + chip, mine_q + 1 - chip, their_q + chip, their_q + 1 - chip]).astype(jnp.int32)

        def quarters(piece, far, axis, after):
            far, _ = lax.optimization_barrier((far, after))
            return join_call(quarters_at, (piece, far, swap_c(piece), swap_c(far)), axis)

        def quarter_cols(v):
            return lax.dynamic_slice_in_dim(v, chip * (v.shape[1] // 2), v.shape[1] // 2, axis=1)


        text_mate0 = swap_x(text_loc[:RB])
        pooled_own = pool_patches(vis_loc)
        pooled_mate = swap_x(pooled_own)
        text_rest, _ = lax.optimization_barrier((text_loc[RB:], pooled_own))
        text_mate1 = swap_x(text_rest)
        dy_src, _ = lax.optimization_barrier((grad_y, text_mate1))
        dy_mate = swap_x(dy_src)

        n_own = pooled_own.shape[0]
        pooled = jnp.where(is_lo, jnp.concatenate([pooled_own, pooled_mate]), jnp.concatenate([pooled_mate, pooled_own]))
        normed, norm_pull = jax.vjp(gain_norm, pooled, pn_gain.astype(F32))
        soft = dot(normed, w_proj).astype(BF16)
        softs = (soft, swap_c(soft))
        normed_c = swap_c(normed)

        qkv_args = (pre1, w_query, w_key, w_value, qg1, kg1, cos_t, sin_t)
        first_rows = qkv_call(meta, (text_loc,), softs, *qkv_args)
        x, hidden, q_raw, q, k_raw, kv = qkv_call(meta, (text_mate0, text_mate1), softs, *qkv_args, prev=first_rows)
        k_all, v_all, kt_all, vt_all = arrange_call(kv_at, kv, swap_c(kv))
        hidden_c = swap_c(hidden)
        o, lse = fwd_call(f_span, q, k_all, vt_all, lim[None])
        y_loc, d_a, d_o, delta, g_post, o_mine, o_theirs = out_call(meta, o, x, grad_y, dy_mate, w_out, post1)
        o_c = swap_c(o_theirs)
        d_a_c = swap_c(d_a)
        delta_t = delta.T[:, None, :]
        dq_mine, dq_theirs, g_qg, dkv_mine, dkv_theirs = bwd_call(b_span, q, d_o, k_all, kt_all, v_all, lim[None], lse, delta_t, q_raw, qg1, cos_t, sin_t)
        dkv_c = swap_c(dkv_theirs)
        dq_c = swap_c(quarter_cols(dq_theirs))
        g_out_q = (tdot(o_mine, d_a) + tdot(o_c, d_a_c)).astype(BF16)
        g_query_q = (tdot(hidden, quarter_cols(dq_mine)) + tdot(hidden_c, dq_c)).astype(BF16)
        dkv_mine, g_out_q, g_query_q = lax.optimization_barrier((dkv_mine, g_out_q, g_query_q))
        g_out_far = swap_x(g_out_q)
        g_query_far = swap_x(g_query_q)
        grad_text, d_merged, dk_raw, d_v, g_pre, g_kg = hid_call(
            meta, dq_mine, dq_theirs, dkv_mine, dkv_c, k_raw, cos_t, sin_t, kg1, w_query, w_key, w_value, x, pre1, grad_y, dy_mate,
            flag_w)

        d_merged_c = swap_c(d_merged)
        kv_c = swap_c(jnp.where(first, d_v, dk_raw))
        g_kv = (tdot(hidden, jnp.where(first, dk_raw, d_v)) + tdot(hidden_c, kv_c)).astype(BF16)
        g_kv_c = swap_c(g_kv)
        g_key, g_value = jnp.where(first, g_kv, g_kv_c), jnp.where(first, g_kv_c, g_kv)

        my_img = jnp.concatenate([2 * lo_dev + jnp.arange(2), 2 * hi_dev + jnp.arange(2)])
        start = img_pos[my_img]
        blk0 = start // RB
        blk1 = jnp.minimum(blk0 + 1, seq // RB - 1)

        def locate(g):
            owner = g // half
            in_set = jnp.minimum(owner, n_dev - 1 - owner)
            return g % half + jnp.where(owner >= n_dev // 2, half, 0), in_set == my_set

        at0, mine0 = locate(blk0)
        at1, mine1 = locate(blk1)
        pick_meta = jnp.stack([at0, at1, start % RB, mine0, mine1, my_set + 0 * start]).astype(jnp.int32)
        d_soft, d_soft_mine, d_soft_theirs = pick_call(pick_meta, d_merged, d_merged_c)
        d_soft_c = swap_c(d_soft_theirs)
        d_normed = dot_t(d_soft, w_proj).astype(BF16)
        d_pooled, g_pn = norm_pull(d_normed)
        g_out = quarters(g_out_q, g_out_far, 0, d_soft)
        g_query = quarters(g_query_q, g_query_far, 1, d_pooled)
        d_own = jnp.where(is_lo, d_pooled[:n_own], d_pooled[n_own:])
        grad_vis = unpool_grad(d_own, vis_loc.shape[0])
        g_proj_half = (tdot(normed, d_soft_mine) + tdot(normed_c, d_soft_c)).astype(BF16)
        g_proj = join_call(halves_at, (g_proj_half, swap_c(g_proj_half)), 1)

        small = jnp.concatenate([g_pn, g_pre[0], g_qg[0], g_kg[0], g_post[0]])
        small = (small + swap_c(small)).astype(BF16)
        cuts = [g_pn.shape[0]]
        for g in (g_pre, g_qg, g_kg):
            cuts.append(cuts[-1] + g.shape[1])
        g_pn, g_pre, g_qg, g_kg, g_post = jnp.split(small, cuts)
        return (y_loc, grad_text, grad_vis, g_pn, g_proj, g_pre, g_query, g_key, g_value, g_qg, g_kg, g_out, g_post)

    in_specs = (seq_spec, seq_spec, part_spec, seq_spec) + (rep_spec,) * 10
    out_specs = (seq_spec, seq_spec, seq_spec) + (part_spec,) * 10

    return jax.shard_map(device_body, mesh=mesh, in_specs=in_specs, out_specs=out_specs, check_vma=False)
```
